256 devices in a mesh: pair: 64 (over z, x_hi, y), occ: 4 (over x_lo, core).
Axes of the slice: x: 4 (x_hi: 2, x_lo: 2; x = x_hi * 2 + x_lo), y: 4, z: 8, core: 2. Of those that a mesh axis runs over, the one named last changes fastest.
Arguments:
- half_ints: bfloat16 [2, 896, 4, 896], P(None, 'pair', 'occ'), may hold values from -6 to 6
- coeffs: bfloat16 [896, 768], P('occ'), may hold values from -0.1875 to 0.1875
- pair_map: int32 [64], replicated, may hold values from 0 to 63, each once
- tile_table: int32 [64], replicated, may hold values from 0 to 63, each once
Outputs:
- mo_ints: float32 [1536, 4, 768], P('pair', 'occ')
The draws below stay inside these ranges and needn't reach their ends.
Inputs may be any that keep to these rules, and one draw needn't show every extreme that they name: pair_map is a permutation of 0 to 63. tile_table is a permutation of 0 to 63.
All inputs are finite; a program needn't handle non-finite values.
Results may differ from the reference program's by a relative error of at most 0.0029.
Values may be sent and summed in bfloat16 or wider, within the bound.
No kernel may reach another device: no remote copies, remote signals or barrier semaphores. Data moves between devices by JAX's collectives and lax.ppermute only.
A program may use at most 64 MiB of HBM per device.

```python
import jax
import jax.numpy as jnp

NBF = 896
NV = 768
I = 2
J = 4
N_PAIR = 64


def shard_levels(stream_key, dims, shards, smallest, largest):
    factor_of = 1.0
    for dim, parts in shards:
        steps = jax.random.uniform(jax.random.fold_in(jax.random.fold_in(stream_key, 6), dim), (parts,), jnp.float32, smallest / len(shards), largest / len(shards))
        factor_of = factor_of * jnp.repeat(jnp.exp(steps), dims[dim] // parts).reshape((-1,) + (1,) * (len(dims) - 1 - dim))
    return factor_of


def bell_draw(stream_key, extent, deviation, most, cuts=(), kind=jnp.bfloat16):
    entries = jax.random.normal(stream_key, extent, jnp.float32) * deviation
    if len(cuts) > 0:
        entries = shard_levels(stream_key, extent, cuts, -0.22, 0.18) * entries
    return jnp.clip(entries, min=-most, max=most).astype(kind)


def setup_inputs(seed: int = 0) -> dict:
    arg_keys = jax.random.split(jax.random.key(seed), 5)
    return {
        "half_ints": bell_draw(arg_keys[0], (I, NBF, J, NBF), 1.0, 6.0, ((1, 64), (2, 4))),
        "coeffs": bell_draw(arg_keys[1], (NBF, NV), NBF ** -0.5, 0.1875, ((0, 4),)),
        "pair_map": jax.random.permutation(arg_keys[2], N_PAIR).astype(jnp.int32),
        "tile_table": jax.random.permutation(arg_keys[3], N_PAIR).astype(jnp.int32),
    }


def reference(half_ints, coeffs, pair_map, tile_table):
    sblock = NBF // N_PAIR
    tile_rows = I * NV // N_PAIR
    split = half_ints.reshape(I, N_PAIR, sblock, J, NBF)
    natural = jnp.zeros_like(split).at[:, pair_map].set(split).reshape(I, NBF, J, NBF)
    half_mo = jnp.einsum("isjr,rb->isjb", natural.astype(jnp.float32), coeffs.astype(jnp.float32)).astype(jnp.bfloat16)
    full = jnp.einsum("sa,isjb->iajb", coeffs.astype(jnp.float32), half_mo.astype(jnp.float32))
    tiles = full.reshape(N_PAIR, tile_rows, J, NV)[tile_table]
    return tiles.reshape(I * NV, J, NV)
```

```python
import jax
import jax.numpy as jnp
from jax import lax
from jax.sharding import Mesh, PartitionSpec as P

S1 = ("z",)
S2 = ("xh", "y")
OCC = ("xl", "c")


def swap(x, axis):
    return lax.ppermute(x, axis, [(0, 1), (1, 0)])


def shards(half_ints, coeffs, pair_map, tile_table):
    num_occ, sblock, _, nbf = half_ints.shape
    nvirt = coeffs.shape[1]
    rows = num_occ * nvirt // 64
    o = lax.axis_index(OCC)
    twin = swap(coeffs, "c")
    far = swap(coeffs, "xl")
    fartwin = swap(far, "c")
    nat = half_ints.reshape(num_occ * sblock, nbf)
    send = jnp.broadcast_to(nat, (8, *nat.shape))
    recv = lax.all_to_all(send, S1, 0, 0, tiled=True)
    full = jnp.zeros((4, *coeffs.shape), coeffs.dtype)
    for piece, k in ((coeffs, o), (twin, o ^ 1), (far, o ^ 2), (fartwin, o ^ 3)):
        full = lax.dynamic_update_index_in_dim(full, piece, k, 0)
    full = full.reshape(nbf, nvirt)
    half = jnp.dot(recv.reshape(-1, nbf), full, preferred_element_type=jnp.float32).astype(jnp.bfloat16)
    half = half.reshape(8, num_occ, sblock, nvirt)
    q = lax.axis_index(S2)
    z = lax.axis_index(S1)
    blocks = pair_map.reshape(8, 8)[:, q]
    tiles = tile_table.reshape(8, 8)[z]
    csel = jnp.take(full.reshape(64, sblock, nvirt), blocks, axis=0)
    cols = jnp.take(csel.reshape(8, sblock, nvirt // rows, rows), tiles % (nvirt // rows), axis=2)
    occ = tiles // (nvirt // rows)
    hot = (occ[:, None] == jnp.arange(num_occ)[None]).astype(jnp.bfloat16)
    left = jnp.einsum("stda,di->dasit", cols, hot).astype(jnp.bfloat16)
    part = jnp.einsum("dasit,sitb->dab", left, half, preferred_element_type=jnp.float32).astype(jnp.bfloat16)
    got = lax.all_to_all(part, S2, 0, 0, tiled=True)
    out = got.astype(jnp.float32).sum(0)
    return out.reshape(rows, 1, nvirt)


def solution(mesh):
    fine = Mesh(mesh.devices.reshape(8, 2, 4, 2, 2), ("z", "xh", "y", "xl", "c"))
    pair = ("z", "xh", "y")
    placed = (P(None, pair, OCC, None), P(OCC, None), P(), P())
    return jax.shard_map(shards, mesh=fine, in_specs=placed, out_specs=P(pair, OCC, None), check_vma=False)
```

```python
import functools

import jax
import jax.numpy as jnp
from jax import lax
from jax.experimental import pallas as pl
from jax.experimental.pallas import tpu as pltpu
from jax.sharding import Mesh, PartitionSpec as P


S1 = ("xh", "y")
S2 = ("z",)
OCC = ("xl", "c")
SIDE = 8


def swap(x, axis):
    return lax.ppermute(x, axis, [(0, 1), (1, 0)])


def hot_kernel(sblock, nocc, cut, pair_map, tile_table, own, full, row_pick, col_pick, mine, pairs, tiles, sems):
    nbf, nvirt = full.shape
    depth = own.shape[0]
    o = lax.axis_index("xl") * 2 + lax.axis_index("c")
    gets = [
        pltpu.make_async_copy(pair_map, pairs, sems.at[0]),
        pltpu.make_async_copy(tile_table, tiles, sems.at[1]),
        pltpu.make_async_copy(own, full.at[pl.ds(pl.multiple_of(o * depth, depth), depth), :], sems.at[2]),
    ]
    for g in gets:
        g.start()
    q = lax.axis_index("xh") * 4 + lax.axis_index("y")
    z = lax.axis_index("z")
    gets[0].wait()
    gets[1].wait()
    span = sblock * nocc
    k = SIDE * span
    r = lax.broadcasted_iota(jnp.int32, (k, 128), 0)
    goal = jnp.zeros((k, 128), jnp.int32)
    for s in range(SIDE):
        goal = jnp.where(r >= s * span, (pairs[z * SIDE + s] - s) * sblock, goal)
    goal = goal + r // nocc - lax.broadcasted_iota(jnp.int32, (k, 128), 1)
    for c in range(nbf // 128):
        row_pick[:, c * 128 : (c + 1) * 128] = (goal == 128 * c).astype(jnp.bfloat16)
    per = nvirt // cut
    lane = lax.broadcasted_iota(jnp.int32, (cut, 128), 1)
    line = lax.broadcasted_iota(jnp.int32, (cut, 128), 0)
    part = lax.broadcasted_iota(jnp.int32, (cut, k), 1) % nocc
    for s in range(SIDE):
        tile = tiles[s * SIDE + q]
        i = tile // per
        goal = (tile - i * per) * cut + line - lane
        at = pl.ds(s * cut, cut)
        for c in range(nvirt // 128):
            col_pick[at, c * 128 : (c + 1) * 128] = (goal == 128 * c).astype(jnp.bfloat16)
        mine[at, :] = (part == i).astype(jnp.float32)
    gets[2].wait()


def pick_kernel(twin, far, fartwin, row_pick, col_pick, mine, had, full, left):
    depth = twin.shape[0]
    o = lax.axis_index("xl") * 2 + lax.axis_index("c")
    for piece, k in ((twin, o ^ 1), (far, o ^ 2), (fartwin, o ^ 3)):
        full[pl.ds(pl.multiple_of(k * depth, depth), depth), :] = piece[...]
    rows = jnp.dot(row_pick[...], full[...], preferred_element_type=jnp.float32).astype(jnp.bfloat16)
    both = lax.dot_general(
        col_pick[...], rows, (((1,), (1,)), ((), ())), preferred_element_type=jnp.float32
    )
    left[...] = (both * mine[...]).astype(jnp.bfloat16)


def copies_kernel(rows, out, held, sem, sems):
    get = pltpu.make_async_copy(rows, held, sem)
    get.start()
    get.wait()
    puts = [pltpu.make_async_copy(held, out.at[k], sems.at[k]) for k in range(SIDE)]
    for c in puts:
        c.start()
    for c in puts:
        c.wait()


def mix_kernel(recv, full, left, part):
    half = jnp.dot(recv[...], full[...], preferred_element_type=jnp.float32).astype(jnp.bfloat16)
    part[...] = jnp.dot(left[...], half, preferred_element_type=jnp.float32).astype(jnp.bfloat16)


def layer(half_ints, coeffs, pair_map, tile_table):
    nocc, sblock, _, nbf = half_ints.shape
    nvirt = coeffs.shape[1]
    cut = nocc * nvirt // lax.axis_size(("z", "xh", "y"))
    vmem = pl.BlockSpec(memory_space=pltpu.VMEM)
    smem = pl.BlockSpec(memory_space=pltpu.SMEM)
    k = SIDE * nocc * sblock
    work = pl.CostEstimate(flops=2 * k * nvirt * (nbf + SIDE * cut), bytes_accessed=0, transcendentals=0)
    small = pltpu.CompilerParams(vmem_limit_bytes=16 << 20)
    far = swap(coeffs, "xl")
    nat = half_ints.transpose(1, 2, 0, 3)
    send = pl.pallas_call(
        copies_kernel,
        out_shape=pltpu.HBM((SIDE, *nat.shape), nat.dtype),
        in_specs=[pl.BlockSpec(memory_space=pltpu.HBM)],
        out_specs=pl.BlockSpec(memory_space=pltpu.HBM),
        scratch_shapes=[pltpu.VMEM(nat.shape, nat.dtype), pltpu.SemaphoreType.DMA, pltpu.SemaphoreType.DMA((SIDE,))],
        compiler_params=small,
        name="copies",
    )(pltpu.with_memory_space_constraint(nat, pltpu.HBM))
    recv = lax.all_to_all(send, S1, 0, 0, tiled=True)
    twin = swap(coeffs, "c")
    fartwin = swap(far, "c")
    hbm = pl.BlockSpec(memory_space=pltpu.HBM)
    own, row_pick, col_pick, mine = pl.pallas_call(
        functools.partial(hot_kernel, sblock, nocc, cut),
        out_shape=(
            jax.ShapeDtypeStruct((nbf, nvirt), jnp.bfloat16),
            jax.ShapeDtypeStruct((k, nbf), jnp.bfloat16),
            jax.ShapeDtypeStruct((SIDE * cut, nvirt), jnp.bfloat16),
            jax.ShapeDtypeStruct((SIDE * cut, k), jnp.float32),
        ),
        in_specs=[hbm] * 3,
        out_specs=(vmem,) * 4,
        scratch_shapes=[
            pltpu.SMEM(pair_map.shape, jnp.int32),
            pltpu.SMEM(tile_table.shape, jnp.int32),
            pltpu.SemaphoreType.DMA((3,)),
        ],
        cost_estimate=work,
        compiler_params=small,
        name="hot",
    )(*(pltpu.with_memory_space_constraint(v, pltpu.HBM) for v in (pair_map, tile_table, coeffs)))
    full, left = pl.pallas_call(
        pick_kernel,
        out_shape=(
            jax.ShapeDtypeStruct((nbf, nvirt), jnp.bfloat16),
            jax.ShapeDtypeStruct((SIDE * cut, k), jnp.bfloat16),
        ),
        in_specs=[vmem] * 7,
        out_specs=(vmem, vmem),
        input_output_aliases={6: 0},
        cost_estimate=work,
        compiler_params=small,
        name="pick",
    )(twin, far, fartwin, row_pick, col_pick, mine, own)
    part = pl.pallas_call(
        mix_kernel,
        out_shape=pltpu.VMEM((SIDE * cut, nvirt), jnp.bfloat16),
        in_specs=[vmem] * 3,
        out_specs=vmem,
        cost_estimate=work,
        compiler_params=small,
        name="mix",
    )(recv.reshape(k, nbf), full, left)
    got = lax.all_to_all(part.reshape(SIDE, cut, nvirt), S2, 0, 0, tiled=True)
    out = got.astype(jnp.float32).sum(0)
    return out.reshape(cut, 1, nvirt)


def solution(mesh):
    fine = Mesh(mesh.devices.reshape(8, 2, 4, 2, 2), ("z", "xh", "y", "xl", "c"))
    pair = ("z", "xh", "y")
    placed = (P(None, pair, OCC, None), P(OCC, None), P(), P())
    return jax.shard_map(layer, mesh=fine, in_specs=placed, out_specs=P(pair, OCC, None), check_vma=False)
```

```python
import functools

import jax
import jax.numpy as jnp
from jax import lax
from jax.experimental import pallas as pl
from jax.experimental.pallas import tpu as pltpu
from jax.sharding import Mesh, PartitionSpec as P


PAIR = ("z", "xh", "y")
PLANE_ORDER = (5, 6, 7, 0, 1, 2, 3, 4)
LINE_ORDER = (5, 1, 6, 2, 7, 3, 0, 4)
OCC = ("xl", "c")
SIDE = 8


def exchange(x, groups):
    return lax.all_to_all(x, PAIR, 0, 0, tiled=True, axis_index_groups=groups)


def swap(x, axis):
    return lax.ppermute(x, axis, [(0, 1), (1, 0)])


def hot_kernel(sblock, nocc, cut, pair_map, tile_table, own, full, row_pick, col_pick, mine, pairs, tiles, sems):
    nbf, nvirt = full.shape
    depth = own.shape[0]
    o = lax.axis_index("xl") * 2 + lax.axis_index("c")
    gets = [
        pltpu.make_async_copy(pair_map, pairs, sems.at[0]),
        pltpu.make_async_copy(tile_table, tiles, sems.at[1]),
        pltpu.make_async_copy(own, full.at[pl.ds(pl.multiple_of(o * depth, depth), depth), :], sems.at[2]),
    ]
    for g in gets:
        g.start()
    q = lax.axis_index("xh") * 4 + lax.axis_index("y")
    z = lax.axis_index("z")
    gets[0].wait()
    gets[1].wait()
    span = sblock * nocc
    k = SIDE * span
    r = lax.broadcasted_iota(jnp.int32, (k, 128), 0)
    goal = jnp.zeros((k, 128), jnp.int32)
    for s in range(SIDE):
        goal = jnp.where(r >= s * span, (pairs[z * SIDE + PLANE_ORDER[s]] - s) * sblock, goal)
    goal = goal + r // nocc - lax.broadcasted_iota(jnp.int32, (k, 128), 1)
    for c in range(nbf // 128):
        row_pick[:, c * 128 : (c + 1) * 128] = (goal == 128 * c).astype(jnp.bfloat16)
    per = nvirt // cut
    lane = lax.broadcasted_iota(jnp.int32, (cut, 128), 1)
    line = lax.broadcasted_iota(jnp.int32, (cut, 128), 0)
    part = lax.broadcasted_iota(jnp.int32, (cut, k), 1) % nocc
    for s in range(SIDE):
        tile = tiles[LINE_ORDER[s] * SIDE + q]
        i = tile // per
        goal = (tile - i * per) * cut + line - lane
        at = pl.ds(s * cut, cut)
        for c in range(nvirt // 128):
            col_pick[at, c * 128 : (c + 1) * 128] = (goal == 128 * c).astype(jnp.bfloat16)
        mine[at, :] = (part == i).astype(jnp.float32)
    gets[2].wait()


def pick_kernel(twin, far, fartwin, row_pick, col_pick, mine, had, full, left):
    depth = twin.shape[0]
    o = lax.axis_index("xl") * 2 + lax.axis_index("c")
    for piece, k in ((twin, o ^ 1), (far, o ^ 2), (fartwin, o ^ 3)):
        full[pl.ds(pl.multiple_of(k * depth, depth), depth), :] = piece[...]
    rows = jnp.dot(row_pick[...], full[...], preferred_element_type=jnp.float32).astype(jnp.bfloat16)
    both = lax.dot_general(
        col_pick[...], rows, (((1,), (1,)), ((), ())), preferred_element_type=jnp.float32
    )
    left[...] = (both * mine[...]).astype(jnp.bfloat16)


def copies_kernel(rows, out, held, sem, sems):
    get = pltpu.make_async_copy(rows, held, sem)
    get.start()
    get.wait()
    puts = [pltpu.make_async_copy(held, out.at[k], sems.at[k]) for k in range(SIDE)]
    for c in puts:
        c.start()
    for c in puts:
        c.wait()


def mix_kernel(recv, full, left, part):
    half = jnp.dot(recv[...], full[...], preferred_element_type=jnp.float32).astype(jnp.bfloat16)
    part[...] = jnp.dot(left[...], half, preferred_element_type=jnp.float32).astype(jnp.bfloat16)


def layer(half_ints, coeffs, pair_map, tile_table):
    nocc, sblock, _, nbf = half_ints.shape
    nvirt = coeffs.shape[1]
    cut = nocc * nvirt // lax.axis_size(PAIR)
    vmem = pl.BlockSpec(memory_space=pltpu.VMEM)
    smem = pl.BlockSpec(memory_space=pltpu.SMEM)
    k = SIDE * nocc * sblock
    work = pl.CostEstimate(flops=2 * k * nvirt * (nbf + SIDE * cut), bytes_accessed=0, transcendentals=0)
    small = pltpu.CompilerParams(vmem_limit_bytes=16 << 20)
    far = swap(coeffs, "xl")
    nat = half_ints.transpose(1, 2, 0, 3)
    send = pl.pallas_call(
        copies_kernel,
        out_shape=pltpu.HBM((SIDE, *nat.shape), nat.dtype),
        in_specs=[pl.BlockSpec(memory_space=pltpu.HBM)],
        out_specs=pl.BlockSpec(memory_space=pltpu.HBM),
        scratch_shapes=[pltpu.VMEM(nat.shape, nat.dtype), pltpu.SemaphoreType.DMA, pltpu.SemaphoreType.DMA((SIDE,))],
        compiler_params=small,
        name="copies",
    )(pltpu.with_memory_space_constraint(nat, pltpu.HBM))
    recv = exchange(send, [[z * SIDE + q for q in PLANE_ORDER] for z in range(SIDE)])
    twin = swap(coeffs, "c")
    fartwin = swap(far, "c")
    hbm = pl.BlockSpec(memory_space=pltpu.HBM)
    own, row_pick, col_pick, mine = pl.pallas_call(
        functools.partial(hot_kernel, sblock, nocc, cut),
        out_shape=(
            jax.ShapeDtypeStruct((nbf, nvirt), jnp.bfloat16),
            jax.ShapeDtypeStruct((k, nbf), jnp.bfloat16),
            jax.ShapeDtypeStruct((SIDE * cut, nvirt), jnp.bfloat16),
            jax.ShapeDtypeStruct((SIDE * cut, k), jnp.float32),
        ),
        in_specs=[hbm] * 3,
        out_specs=(vmem,) * 4,
        scratch_shapes=[
            pltpu.SMEM(pair_map.shape, jnp.int32),
            pltpu.SMEM(tile_table.shape, jnp.int32),
            pltpu.SemaphoreType.DMA((3,)),
        ],
        cost_estimate=work,
        compiler_params=small,
        name="hot",
    )(*(pltpu.with_memory_space_constraint(v, pltpu.HBM) for v in (pair_map, tile_table, coeffs)))
    full, left = pl.pallas_call(
        pick_kernel,
        out_shape=(
            jax.ShapeDtypeStruct((nbf, nvirt), jnp.bfloat16),
            jax.ShapeDtypeStruct((SIDE * cut, k), jnp.bfloat16),
        ),
        in_specs=[vmem] * 7,
        out_specs=(vmem, vmem),
        input_output_aliases={6: 0},
        cost_estimate=work,
        compiler_params=small,
        name="pick",
    )(twin, far, fartwin, row_pick, col_pick, mine, own)
    part = pl.pallas_call(
        mix_kernel,
        out_shape=pltpu.VMEM((SIDE * cut, nvirt), jnp.bfloat16),
        in_specs=[vmem] * 3,
        out_specs=vmem,
        cost_estimate=work,
        compiler_params=small,
        name="mix",
    )(recv.reshape(k, nbf), full, left)
    got = exchange(part.reshape(SIDE, cut, nvirt), [[z * SIDE + q for z in LINE_ORDER] for q in range(SIDE)])
    out = got.astype(jnp.float32).sum(0)
    return out.reshape(cut, 1, nvirt)


def solution(mesh):
    fine = Mesh(mesh.devices.reshape(8, 2, 4, 2, 2), ("z", "xh", "y", "xl", "c"))
    placed = (P(None, PAIR, OCC, None), P(OCC, None), P(), P())
    return jax.shard_map(layer, mesh=fine, in_specs=placed, out_specs=P(PAIR, OCC, None), check_vma=False)
```

```python
import functools

import jax
import jax.numpy as jnp
from jax import lax
from jax.experimental import pallas as pl
from jax.experimental.pallas import tpu as pltpu
from jax.sharding import Mesh, PartitionSpec as P


PAIR = ("z", "xh", "y")
PLANE_FIRST = 0
PLANE_ORDER = (5, 6, 7, 0, 1, 2, 3, 4)
LINE_ORDER = (5, 1, 6, 2, 7, 3, 0, 4)
OCC = ("xl", "c")
SIDE = 8


def exchange(x, plane_core):
    groups = []
    for fixed in range(SIDE):
        for xl in range(2):
            plane = [(fixed * SIDE + q) * 4 + xl * 2 + plane_core for q in PLANE_ORDER]
            line = [(z * SIDE + fixed) * 4 + xl * 2 + 1 - plane_core for z in LINE_ORDER]
            groups += [plane, line]
    return lax.all_to_all(x, PAIR + OCC, 0, 0, tiled=True, axis_index_groups=groups)


def swap(x, axis):
    return lax.ppermute(x, axis, [(0, 1), (1, 0)])


def hot_kernel(sblock, nocc, cut, pair_map, tile_table, own, full, row_pick, col_pick, mine, pairs, tiles, sems):
    nbf, nvirt = full.shape
    depth = own.shape[0]
    o = lax.axis_index("xl") * 2 + lax.axis_index("c")
    gets = [
        pltpu.make_async_copy(pair_map, pairs, sems.at[0]),
        pltpu.make_async_copy(tile_table, tiles, sems.at[1]),
        pltpu.make_async_copy(own, full.at[pl.ds(pl.multiple_of(o * depth, depth), depth), :], sems.at[2]),
    ]
    for g in gets:
        g.start()
    q = lax.axis_index("xh") * 4 + lax.axis_index("y")
    z = lax.axis_index("z")
    plane_first = lax.axis_index("c") == PLANE_FIRST
    gets[0].wait()
    gets[1].wait()
    span = sblock * nocc
    k = SIDE * span
    r = lax.broadcasted_iota(jnp.int32, (k, 128), 0)
    goal = jnp.zeros((k, 128), jnp.int32)
    for s in range(SIDE):
        source = jnp.where(plane_first, z * SIDE + PLANE_ORDER[s], LINE_ORDER[s] * SIDE + q)
        goal = jnp.where(r >= s * span, (pairs[source] - s) * sblock, goal)
    goal = goal + r // nocc - lax.broadcasted_iota(jnp.int32, (k, 128), 1)
    for c in range(nbf // 128):
        row_pick[:, c * 128 : (c + 1) * 128] = (goal == 128 * c).astype(jnp.bfloat16)
    per = nvirt // cut
    lane = lax.broadcasted_iota(jnp.int32, (cut, 128), 1)
    line = lax.broadcasted_iota(jnp.int32, (cut, 128), 0)
    part = lax.broadcasted_iota(jnp.int32, (cut, k), 1) % nocc
    for s in range(SIDE):
        tile = tiles[jnp.where(plane_first, LINE_ORDER[s] * SIDE + q, z * SIDE + PLANE_ORDER[s])]
        i = tile // per
        goal = (tile - i * per) * cut + line - lane
        at = pl.ds(s * cut, cut)
        for c in range(nvirt // 128):
            col_pick[at, c * 128 : (c + 1) * 128] = (goal == 128 * c).astype(jnp.bfloat16)
        mine[at, :] = (part == i).astype(jnp.float32)
    gets[2].wait()


def pick_kernel(twin, far, fartwin, row_pick, col_pick, mine, had, full, left):
    depth = twin.shape[0]
    o = lax.axis_index("xl") * 2 + lax.axis_index("c")
    for piece, k in ((twin, o ^ 1), (far, o ^ 2), (fartwin, o ^ 3)):
        full[pl.ds(pl.multiple_of(k * depth, depth), depth), :] = piece[...]
    rows = jnp.dot(row_pick[...], full[...], preferred_element_type=jnp.float32).astype(jnp.bfloat16)
    both = lax.dot_general(
        col_pick[...], rows, (((1,), (1,)), ((), ())), preferred_element_type=jnp.float32
    )
    left[...] = (both * mine[...]).astype(jnp.bfloat16)


def copies_kernel(rows, out, held, sem, sems):
    get = pltpu.make_async_copy(rows, held, sem)
    get.start()
    get.wait()
    puts = [pltpu.make_async_copy(held, out.at[k], sems.at[k]) for k in range(SIDE)]
    for c in puts:
        c.start()
    for c in puts:
        c.wait()


def mix_kernel(recv, full, left, part):
    half = jnp.dot(recv[...], full[...], preferred_element_type=jnp.float32).astype(jnp.bfloat16)
    part[...] = jnp.dot(left[...], half, preferred_element_type=jnp.float32).astype(jnp.bfloat16)


def layer(half_ints, coeffs, pair_map, tile_table):
    nocc, sblock, _, nbf = half_ints.shape
    nvirt = coeffs.shape[1]
    cut = nocc * nvirt // lax.axis_size(PAIR)
    vmem = pl.BlockSpec(memory_space=pltpu.VMEM)
    smem = pl.BlockSpec(memory_space=pltpu.SMEM)
    k = SIDE * nocc * sblock
    work = pl.CostEstimate(flops=2 * k * nvirt * (nbf + SIDE * cut), bytes_accessed=0, transcendentals=0)
    small = pltpu.CompilerParams(vmem_limit_bytes=16 << 20)
    far = swap(coeffs, "xl")
    nat = half_ints.transpose(1, 2, 0, 3)
    send = pl.pallas_call(
        copies_kernel,
        out_shape=pltpu.HBM((SIDE, *nat.shape), nat.dtype),
        in_specs=[pl.BlockSpec(memory_space=pltpu.HBM)],
        out_specs=pl.BlockSpec(memory_space=pltpu.HBM),
        scratch_shapes=[pltpu.VMEM(nat.shape, nat.dtype), pltpu.SemaphoreType.DMA, pltpu.SemaphoreType.DMA((SIDE,))],
        compiler_params=small,
        name="copies",
    )(pltpu.with_memory_space_constraint(nat, pltpu.HBM))
    recv = exchange(send, PLANE_FIRST)
    twin = swap(coeffs, "c")
    fartwin = swap(far, "c")
    hbm = pl.BlockSpec(memory_space=pltpu.HBM)
    own, row_pick, col_pick, mine = pl.pallas_call(
        functools.partial(hot_kernel, sblock, nocc, cut),
        out_shape=(
            jax.ShapeDtypeStruct((nbf, nvirt), jnp.bfloat16),
            jax.ShapeDtypeStruct((k, nbf), jnp.bfloat16),
            jax.ShapeDtypeStruct((SIDE * cut, nvirt), jnp.bfloat16),
            jax.ShapeDtypeStruct((SIDE * cut, k), jnp.float32),
        ),
        in_specs=[hbm] * 3,
        out_specs=(vmem,) * 4,
        scratch_shapes=[
            pltpu.SMEM(pair_map.shape, jnp.int32),
            pltpu.SMEM(tile_table.shape, jnp.int32),
            pltpu.SemaphoreType.DMA((3,)),
        ],
        cost_estimate=work,
        compiler_params=small,
        name="hot",
    )(*(pltpu.with_memory_space_constraint(v, pltpu.HBM) for v in (pair_map, tile_table, coeffs)))
    full, left = pl.pallas_call(
        pick_kernel,
        out_shape=(
            jax.ShapeDtypeStruct((nbf, nvirt), jnp.bfloat16),
            jax.ShapeDtypeStruct((SIDE * cut, k), jnp.bfloat16),
        ),
        in_specs=[vmem] * 7,
        out_specs=(vmem, vmem),
        input_output_aliases={6: 0},
        cost_estimate=work,
        compiler_params=small,
        name="pick",
    )(twin, far, fartwin, row_pick, col_pick, mine, own)
    part = pl.pallas_call(
        mix_kernel,
        out_shape=pltpu.VMEM((SIDE * cut, nvirt), jnp.bfloat16),
        in_specs=[vmem] * 3,
        out_specs=vmem,
        cost_estimate=work,
        compiler_params=small,
        name="mix",
    )(recv.reshape(k, nbf), full, left)
    got = exchange(part.reshape(SIDE, cut, nvirt), 1 - PLANE_FIRST)
    out = got.astype(jnp.float32).sum(0)
    return out.reshape(cut, 1, nvirt)


def solution(mesh):
    fine = Mesh(mesh.devices.reshape(8, 2, 4, 2, 2), ("z", "xh", "y", "xl", "c"))
    placed = (P(None, PAIR, OCC, None), P(OCC, None), P(), P())
    return jax.shard_map(layer, mesh=fine, in_specs=placed, out_specs=P(PAIR, OCC, None), check_vma=False)
```

```python
import functools

import jax
import jax.numpy as jnp
from jax import lax
from jax.experimental import pallas as pl
from jax.experimental.pallas import tpu as pltpu
from jax.sharding import Mesh, PartitionSpec as P


PAIR = ("z", "xh", "y")
PLANE_FIRST = 0
FIRST_PLANES = (7, 6, 5, 4, 3, 2, 1, 0)
NEXT_PLANES = (5, 6, 7, 0, 1, 2, 3, 4)
FIRST_LINES = (5, 1, 6, 2, 7, 3, 0, 4)
NEXT_LINES = (5, 1, 6, 2, 7, 3, 0, 4)
OCC = ("xl", "c")
SIDE = 8


def exchange(x, plane_core, plane_order, line_order):
    groups = []
    for fixed in range(SIDE):
        for xl in range(2):
            plane = [(fixed * SIDE + q) * 4 + xl * 2 + plane_core for q in plane_order]
            line = [(z * SIDE + fixed) * 4 + xl * 2 + 1 - plane_core for z in line_order]
            groups += [plane, line]
    return lax.all_to_all(x, PAIR + OCC, 0, 0, tiled=True, axis_index_groups=groups)


def swap(x, axis):
    return lax.ppermute(x, axis, [(0, 1), (1, 0)])


def hot_kernel(sblock, nocc, cut, pair_map, tile_table, own, full, row_pick, col_pick, mine, pairs, tiles, sems):
    nbf, nvirt = full.shape
    depth = own.shape[0]
    o = lax.axis_index("xl") * 2 + lax.axis_index("c")
    gets = [
        pltpu.make_async_copy(pair_map, pairs, sems.at[0]),
        pltpu.make_async_copy(tile_table, tiles, sems.at[1]),
        pltpu.make_async_copy(own, full.at[pl.ds(pl.multiple_of(o * depth, depth), depth), :], sems.at[2]),
    ]
    for g in gets:
        g.start()
    q = lax.axis_index("xh") * 4 + lax.axis_index("y")
    z = lax.axis_index("z")
    plane_first = lax.axis_index("c") == PLANE_FIRST
    gets[0].wait()
    gets[1].wait()
    span = sblock * nocc
    k = SIDE * span
    r = lax.broadcasted_iota(jnp.int32, (k, 128), 0)
    goal = jnp.zeros((k, 128), jnp.int32)
    for s in range(SIDE):
        source = jnp.where(plane_first, z * SIDE + FIRST_PLANES[s], FIRST_LINES[s] * SIDE + q)
        goal = jnp.where(r >= s * span, (pairs[source] - s) * sblock, goal)
    goal = goal + r // nocc - lax.broadcasted_iota(jnp.int32, (k, 128), 1)
    for c in range(nbf // 128):
        row_pick[:, c * 128 : (c + 1) * 128] = (goal == 128 * c).astype(jnp.bfloat16)
    per = nvirt // cut
    lane = lax.broadcasted_iota(jnp.int32, (cut, 128), 1)
    line = lax.broadcasted_iota(jnp.int32, (cut, 128), 0)
    part = lax.broadcasted_iota(jnp.int32, (cut, k), 1) % nocc
    for s in range(SIDE):
        tile = tiles[jnp.where(plane_first, NEXT_LINES[s] * SIDE + q, z * SIDE + NEXT_PLANES[s])]
        i = tile // per
        goal = (tile - i * per) * cut + line - lane
        at = pl.ds(s * cut, cut)
        for c in range(nvirt // 128):
            col_pick[at, c * 128 : (c + 1) * 128] = (goal == 128 * c).astype(jnp.bfloat16)
        mine[at, :] = (part == i).astype(jnp.float32)
    gets[2].wait()


def pick_kernel(twin, far, fartwin, row_pick, col_pick, mine, had, full, left):
    depth = twin.shape[0]
    o = lax.axis_index("xl") * 2 + lax.axis_index("c")
    for piece, k in ((twin, o ^ 1), (far, o ^ 2), (fartwin, o ^ 3)):
        full[pl.ds(pl.multiple_of(k * depth, depth), depth), :] = piece[...]
    rows = jnp.dot(row_pick[...], full[...], preferred_element_type=jnp.float32).astype(jnp.bfloat16)
    both = lax.dot_general(
        col_pick[...], rows, (((1,), (1,)), ((), ())), preferred_element_type=jnp.float32
    )
    left[...] = (both * mine[...]).astype(jnp.bfloat16)


def copies_kernel(rows, out, held, sem, sems):
    get = pltpu.make_async_copy(rows, held, sem)
    get.start()
    get.wait()
    puts = [pltpu.make_async_copy(held, out.at[k], sems.at[k]) for k in range(SIDE)]
    for c in puts:
        c.start()
    for c in puts:
        c.wait()


def mix_kernel(recv, full, left, part):
    half = jnp.dot(recv[...].reshape(-1, full.shape[0]), full[...], preferred_element_type=jnp.float32).astype(jnp.bfloat16)
    part[...] = jnp.dot(left[...], half, preferred_element_type=jnp.float32).astype(jnp.bfloat16)


def layer(half_ints, coeffs, pair_map, tile_table):
    nocc, sblock, _, nbf = half_ints.shape
    nvirt = coeffs.shape[1]
    cut = nocc * nvirt // lax.axis_size(PAIR)
    vmem = pl.BlockSpec(memory_space=pltpu.VMEM)
    smem = pl.BlockSpec(memory_space=pltpu.SMEM)
    k = SIDE * nocc * sblock
    work = pl.CostEstimate(flops=2 * k * nvirt * (nbf + SIDE * cut), bytes_accessed=0, transcendentals=0)
    small = pltpu.CompilerParams(vmem_limit_bytes=16 << 20)
    far = swap(coeffs, "xl")
    nat = half_ints.transpose(1, 2, 0, 3)
    send = pl.pallas_call(
        copies_kernel,
        out_shape=pltpu.HBM((SIDE, *nat.shape), nat.dtype),
        in_specs=[pl.BlockSpec(memory_space=pltpu.HBM)],
        out_specs=pl.BlockSpec(memory_space=pltpu.HBM),
        scratch_shapes=[pltpu.VMEM(nat.shape, nat.dtype), pltpu.SemaphoreType.DMA, pltpu.SemaphoreType.DMA((SIDE,))],
        compiler_params=small,
        name="copies",
    )(pltpu.with_memory_space_constraint(nat, pltpu.HBM))
    recv = exchange(send, PLANE_FIRST, FIRST_PLANES, FIRST_LINES)
    twin = swap(coeffs, "c")
    fartwin = swap(far, "c")
    hbm = pl.BlockSpec(memory_space=pltpu.HBM)
    own, row_pick, col_pick, mine = pl.pallas_call(
        functools.partial(hot_kernel, sblock, nocc, cut),
        out_shape=(
            jax.ShapeDtypeStruct((nbf, nvirt), jnp.bfloat16),
            jax.ShapeDtypeStruct((k, nbf), jnp.bfloat16),
            jax.ShapeDtypeStruct((SIDE * cut, nvirt), jnp.bfloat16),
            jax.ShapeDtypeStruct((SIDE * cut, k), jnp.float32),
        ),
        in_specs=[hbm] * 3,
        out_specs=(vmem,) * 4,
        scratch_shapes=[
            pltpu.SMEM(pair_map.shape, jnp.int32),
            pltpu.SMEM(tile_table.shape, jnp.int32),
            pltpu.SemaphoreType.DMA((3,)),
        ],
        cost_estimate=work,
        compiler_params=small,
        name="hot",
    )(*(pltpu.with_memory_space_constraint(v, pltpu.HBM) for v in (pair_map, tile_table, coeffs)))
    full, left = pl.pallas_call(
        pick_kernel,
        out_shape=(
            jax.ShapeDtypeStruct((nbf, nvirt), jnp.bfloat16),
            jax.ShapeDtypeStruct((SIDE * cut, k), jnp.bfloat16),
        ),
        in_specs=[vmem] * 7,
        out_specs=(vmem, vmem),
        input_output_aliases={6: 0},
        cost_estimate=work,
        compiler_params=small,
        name="pick",
    )(twin, far, fartwin, row_pick, col_pick, mine, own)
    part = pl.pallas_call(
        mix_kernel,
        out_shape=pltpu.VMEM((SIDE * cut, nvirt), jnp.bfloat16),
        in_specs=[vmem] * 3,
        out_specs=vmem,
        cost_estimate=work,
        compiler_params=small,
        name="mix",
    )(recv.reshape(SIDE, sblock, nocc, nbf), full, left)
    got = exchange(part.reshape(SIDE, cut, nvirt), 1 - PLANE_FIRST, NEXT_PLANES, NEXT_LINES)
    out = got.astype(jnp.float32).sum(0)
    return out.reshape(cut, 1, nvirt)


def solution(mesh):
    fine = Mesh(mesh.devices.reshape(8, 2, 4, 2, 2), ("z", "xh", "y", "xl", "c"))
    placed = (P(None, PAIR, OCC, None), P(OCC, None), P(), P())
    return jax.shard_map(layer, mesh=fine, in_specs=placed, out_specs=P(PAIR, OCC, None), check_vma=False)
```

```python
import functools

import jax
import jax.numpy as jnp
from jax import lax
from jax.experimental import pallas as pl
from jax.experimental.pallas import tpu as pltpu
from jax.sharding import Mesh, PartitionSpec as P


PAIR = ("z", "xh", "y")
PLANE_FIRST = 1
FIRST_PLANES = (2, 3, 4, 5, 6, 7, 0, 1)
NEXT_PLANES = (6, 7, 0, 1, 2, 3, 4, 5)
FIRST_LINES = (5, 1, 6, 2, 7, 3, 0, 4)
NEXT_LINES = (5, 1, 6, 2, 7, 3, 0, 4)
OCC = ("xl", "c")
SIDE = 8


def exchange(x, plane_core, plane_order, line_order):
    groups = []
    for fixed in range(SIDE):
        for xl in range(2):
            plane = [(fixed * SIDE + q) * 4 + xl * 2 + plane_core for q in plane_order]
            line = [(z * SIDE + fixed) * 4 + xl * 2 + 1 - plane_core for z in line_order]
            groups += [plane, line]
    return lax.all_to_all(x, PAIR + OCC, 0, 0, tiled=True, axis_index_groups=groups)


def swap(x, axis):
    return lax.ppermute(x, axis, [(0, 1), (1, 0)])


def hot_kernel(sblock, nocc, cut, pair_map, tile_table, own, full, row_pick, col_pick, mine, pairs, tiles, sems):
    nbf, nvirt = full.shape
    depth = own.shape[0]
    o = lax.axis_index("xl") * 2 + lax.axis_index("c")
    gets = [
        pltpu.make_async_copy(pair_map, pairs, sems.at[0]),
        pltpu.make_async_copy(tile_table, tiles, sems.at[1]),
        pltpu.make_async_copy(own, full.at[pl.ds(pl.multiple_of(o * depth, depth), depth), :], sems.at[2]),
    ]
    for g in gets:
        g.start()
    q = lax.axis_index("xh") * 4 + lax.axis_index("y")
    z = lax.axis_index("z")
    plane_first = lax.axis_index("c") == PLANE_FIRST
    gets[0].wait()
    gets[1].wait()
    span = sblock * nocc
    k = SIDE * span
    r = lax.broadcasted_iota(jnp.int32, (k, 128), 0)
    goal = jnp.zeros((k, 128), jnp.int32)
    for s in range(SIDE):
        source = jnp.where(plane_first, z * SIDE + FIRST_PLANES[s], FIRST_LINES[s] * SIDE + q)
        goal = jnp.where(r >= s * span, (pairs[source] - s) * sblock, goal)
    goal = goal + r // nocc - lax.broadcasted_iota(jnp.int32, (k, 128), 1)
    for c in range(nbf // 128):
        row_pick[:, c * 128 : (c + 1) * 128] = (goal == 128 * c).astype(jnp.bfloat16)
    per = nvirt // cut
    lane = lax.broadcasted_iota(jnp.int32, (cut, 128), 1)
    line = lax.broadcasted_iota(jnp.int32, (cut, 128), 0)
    part = lax.broadcasted_iota(jnp.int32, (cut, k), 1) % nocc
    for s in range(SIDE):
        tile = tiles[jnp.where(plane_first, NEXT_LINES[s] * SIDE + q, z * SIDE + NEXT_PLANES[s])]
        i = tile // per
        goal = (tile - i * per) * cut + line - lane
        at = pl.ds(s * cut, cut)
        for c in range(nvirt // 128):
            col_pick[at, c * 128 : (c + 1) * 128] = (goal == 128 * c).astype(jnp.bfloat16)
        mine[at, :] = (part == i).astype(jnp.float32)
    gets[2].wait()


def pick_kernel(twin, far, fartwin, row_pick, col_pick, mine, had, full, left):
    depth = twin.shape[0]
    o = lax.axis_index("xl") * 2 + lax.axis_index("c")
    for piece, k in ((twin, o ^ 1), (far, o ^ 2), (fartwin, o ^ 3)):
        full[pl.ds(pl.multiple_of(k * depth, depth), depth), :] = piece[...]
    rows = jnp.dot(row_pick[...], full[...], preferred_element_type=jnp.float32).astype(jnp.bfloat16)
    both = lax.dot_general(
        col_pick[...], rows, (((1,), (1,)), ((), ())), preferred_element_type=jnp.float32
    )
    left[...] = (both * mine[...]).astype(jnp.bfloat16)


def copies_kernel(rows, out, sems):
    puts = [pltpu.make_async_copy(rows, out.at[k], sems.at[k]) for k in range(SIDE)]
    for c in puts:
        c.start()
    for c in puts:
        c.wait()


def mix_kernel(recv, full, left, part):
    half = jnp.dot(recv[...].reshape(-1, full.shape[0]), full[...], preferred_element_type=jnp.float32).astype(jnp.bfloat16)
    part[...] = jnp.dot(left[...], half, preferred_element_type=jnp.float32).astype(jnp.bfloat16)


def layer(half_ints, coeffs, pair_map, tile_table):
    nocc, sblock, _, nbf = half_ints.shape
    nvirt = coeffs.shape[1]
    cut = nocc * nvirt // lax.axis_size(PAIR)
    vmem = pl.BlockSpec(memory_space=pltpu.VMEM)
    smem = pl.BlockSpec(memory_space=pltpu.SMEM)
    k = SIDE * nocc * sblock
    work = pl.CostEstimate(flops=2 * k * nvirt * (nbf + SIDE * cut), bytes_accessed=0, transcendentals=0)
    small = pltpu.CompilerParams(vmem_limit_bytes=16 << 20)
    far = swap(coeffs, "xl")
    nat = half_ints.transpose(1, 2, 0, 3)
    send = pl.pallas_call(
        copies_kernel,
        out_shape=pltpu.HBM((SIDE, *nat.shape), nat.dtype),
        in_specs=[vmem],
        out_specs=pl.BlockSpec(memory_space=pltpu.HBM),
        scratch_shapes=[
            pltpu.SemaphoreType.DMA((SIDE,)),
        ],
        compiler_params=small,
        name="copies",
    )(nat)
    recv = exchange(send, PLANE_FIRST, FIRST_PLANES, FIRST_LINES)
    twin = swap(coeffs, "c")
    fartwin = swap(far, "c")
    hbm = pl.BlockSpec(memory_space=pltpu.HBM)
    own, row_pick, col_pick, mine = pl.pallas_call(
        functools.partial(hot_kernel, sblock, nocc, cut),
        out_shape=(
            jax.ShapeDtypeStruct((nbf, nvirt), jnp.bfloat16),
            jax.ShapeDtypeStruct((k, nbf), jnp.bfloat16),
            jax.ShapeDtypeStruct((SIDE * cut, nvirt), jnp.bfloat16),
            jax.ShapeDtypeStruct((SIDE * cut, k), jnp.float32),
        ),
        in_specs=[hbm] * 3,
        out_specs=(vmem,) * 4,
        scratch_shapes=[
            pltpu.SMEM(pair_map.shape, jnp.int32),
            pltpu.SMEM(tile_table.shape, jnp.int32),
            pltpu.SemaphoreType.DMA((3,)),
        ],
        cost_estimate=work,
        compiler_params=small,
        name="hot",
    )(*(pltpu.with_memory_space_constraint(v, pltpu.HBM) for v in (pair_map, tile_table, coeffs)))
    full, left = pl.pallas_call(
        pick_kernel,
        out_shape=(
            jax.ShapeDtypeStruct((nbf, nvirt), jnp.bfloat16),
            jax.ShapeDtypeStruct((SIDE * cut, k), jnp.bfloat16),
        ),
        in_specs=[vmem] * 7,
        out_specs=(vmem, vmem),
        input_output_aliases={6: 0},
        cost_estimate=work,
        compiler_params=small,
        name="pick",
    )(twin, far, fartwin, row_pick, col_pick, mine, own)
    part = pl.pallas_call(
        mix_kernel,
        out_shape=pltpu.VMEM((SIDE * cut, nvirt), jnp.bfloat16),
        in_specs=[vmem] * 3,
        out_specs=vmem,
        cost_estimate=work,
        compiler_params=small,
        name="mix",
    )(recv.reshape(SIDE, sblock, nocc, nbf), full, left)
    got = exchange(part.reshape(SIDE, cut, nvirt), 1 - PLANE_FIRST, NEXT_PLANES, NEXT_LINES)
    out = got.astype(jnp.float32).sum(0)
    return out.reshape(cut, 1, nvirt)


def solution(mesh):
    fine = Mesh(mesh.devices.reshape(8, 2, 4, 2, 2), ("z", "xh", "y", "xl", "c"))
    placed = (P(None, PAIR, OCC, None), P(OCC, None), P(), P())
    return jax.shard_map(layer, mesh=fine, in_specs=placed, out_specs=P(PAIR, OCC, None), check_vma=False)
```
